32 devices in a mesh: rep: 1, dp: 32 (over x, y, z, core).
Axes of the slice: x: 2, y: 2, z: 4, core: 2. Of those that a mesh axis runs over, the one named last changes fastest.
Arguments:
- x: bfloat16 [32, 2048, 512], P(('rep', 'dp'))
- dy: bfloat16 [32, 2048, 512], P(('rep', 'dp'))
- wq: bfloat16 [2, 512, 512], replicated
- wk: bfloat16 [2, 512, 512], replicated
- wv: bfloat16 [2, 512, 512], replicated
- wo: bfloat16 [2, 512, 512], replicated
- w_gate: bfloat16 [2, 512, 2048], replicated
- w_up: bfloat16 [2, 512, 2048], replicated
- w_down: bfloat16 [2, 2048, 512], replicated
- m_wq: float32 [2, 512, 512], replicated
- m_wk: float32 [2, 512, 512], replicated
- m_wv: float32 [2, 512, 512], replicated
- m_wo: float32 [2, 512, 512], replicated
- m_w_gate: float32 [2, 512, 2048], replicated
- m_w_up: float32 [2, 512, 2048], replicated
- m_w_down: float32 [2, 2048, 512], replicated
- v_wq: float32 [2, 512, 512], replicated
- v_wk: float32 [2, 512, 512], replicated
- v_wv: float32 [2, 512, 512], replicated
- v_wo: float32 [2, 512, 512], replicated
- v_w_gate: float32 [2, 512, 2048], replicated
- v_w_up: float32 [2, 512, 2048], replicated
- v_w_down: float32 [2, 2048, 512], replicated
Outputs:
- output 1: bfloat16 [2, 512, 512], P('rep')
- output 2: bfloat16 [2, 512, 512], P('rep')
- output 3: bfloat16 [2, 512, 512], P('rep')
- output 4: bfloat16 [2, 512, 512], P('rep')
- output 5: bfloat16 [2, 512, 2048], P('rep')
- output 6: bfloat16 [2, 512, 2048], P('rep')
- output 7: bfloat16 [2, 2048, 512], P('rep')
- output 8: float32 [2, 512, 512], P('rep')
- output 9: float32 [2, 512, 512], P('rep')
- output 10: float32 [2, 512, 512], P('rep')
- output 11: float32 [2, 512, 512], P('rep')
- output 12: float32 [2, 512, 2048], P('rep')
- output 13: float32 [2, 512, 2048], P('rep')
- output 14: float32 [2, 2048, 512], P('rep')
- output 15: float32 [2, 512, 512], P('rep')
- output 16: float32 [2, 512, 512], P('rep')
- output 17: float32 [2, 512, 512], P('rep')
- output 18: float32 [2, 512, 512], P('rep')
- output 19: float32 [2, 512, 2048], P('rep')
- output 20: float32 [2, 512, 2048], P('rep')
- output 21: float32 [2, 2048, 512], P('rep')
All inputs are finite; a program needn't handle non-finite values.
Results may differ from the reference program's by a relative error of at most 0.024.
Values are sent between devices in bfloat16 or wider.
A program may use at most 2.25 GiB of HBM per device.

```python
import jax
import jax.numpy as jnp
from jax import lax

SEQUENCES = 32
TOKENS = 2048
D = 512
HEADS = 4
KV_HEADS = 4
HEAD = 128
FF = 2048
LAYERS = 2
THETA = 10000
NAMES = ("wq", "wk", "wv", "wo", "w_gate", "w_up", "w_down")
SHAPES = {
    "wq": (LAYERS, D, HEADS * HEAD),
    "wk": (LAYERS, D, KV_HEADS * HEAD),
    "wv": (LAYERS, D, KV_HEADS * HEAD),
    "wo": (LAYERS, HEADS * HEAD, D),
    "w_gate": (LAYERS, D, FF),
    "w_up": (LAYERS, D, FF),
    "w_down": (LAYERS, FF, D),
}


def bump(key, n, height):
    away = (jnp.arange(n, dtype=jnp.int32) - jax.random.randint(key, (), 0, n, jnp.int32)) % n
    return jnp.where(away < n // 8, height, 1.0)


def together(key, own, strength):
    shared = jax.random.normal(key, own.shape[1:], jnp.float32)
    return (own + strength * shared) * lax.rsqrt(1 + strength * strength)


def setup_inputs(seed: int = 0, part: int = 0) -> dict:
    kx, kdy, ka, kb, kz, kf, kh, kl, *keys = jax.random.split(jax.random.key(seed), 8 + 3 * len(NAMES))
    kx, kdy, ka, kb = (jax.random.fold_in(k, part) for k in (kx, kdy, ka, kb))
    kw, km, kv = (keys[i::3] for i in range(3))
    shape = (SEQUENCES, TOKENS, D)
    much_x, much_dy = jax.random.uniform(kz, (2,), jnp.float32, 0.0, 1.0)
    loud = 2.0 ** jax.random.uniform(jax.random.fold_in(kz, 1), (), jnp.float32, -1.0, 2.0)
    layers = 2.0 ** jax.random.uniform(kl, (LAYERS, 1, 1), jnp.float32, -1.0, 1.0)
    times = {"wq": 1.0, "wk": 1.0, "wv": 2.0, "wo": layers, "w_gate": 1.0, "w_up": bump(kh, FF, 4.0), "w_down": layers}
    x = together(ka, jax.random.normal(kx, shape, jnp.float32), much_x) * bump(kf, D, 4.0)
    dy = together(kb, jax.random.normal(kdy, shape, jnp.float32), much_dy)
    drawn = {"x": x.astype(jnp.bfloat16), "dy": (loud * dy * (SEQUENCES * TOKENS) ** -0.5).astype(jnp.bfloat16)}
    for key, name in zip(kw, NAMES, strict=True):
        drawn[name] = (jax.random.normal(key, SHAPES[name], jnp.float32) * SHAPES[name][1] ** -0.5 * times[name]).astype(jnp.bfloat16)
    for key, name in zip(km, NAMES, strict=True):
        drawn[f"m_{name}"] = 0.1 * jax.random.normal(key, SHAPES[name], jnp.float32)
    for key, name in zip(kv, NAMES, strict=True):
        drawn[f"v_{name}"] = jax.random.uniform(key, SHAPES[name], jnp.float32, 0.02, 0.06)
    return drawn


def matmul(a, w):
    return jnp.dot(a, w, preferred_element_type=jnp.float32).astype(jnp.bfloat16)


def normed(h):
    wide = h.astype(jnp.float32)
    scale = lax.rsqrt(jnp.mean(wide**2, -1, keepdims=True) + 1e-6)
    return (wide * scale).astype(jnp.bfloat16)


def turned(t, theta):
    half = t.shape[-1] // 2
    angle = jnp.arange(t.shape[0], dtype=jnp.float32)[:, None] * theta ** (-jnp.arange(half, dtype=jnp.float32) / half)
    cos, sin = jnp.cos(angle)[:, None], jnp.sin(angle)[:, None]
    a, b = t[..., :half].astype(jnp.float32), t[..., half:].astype(jnp.float32)
    return jnp.concatenate([a * cos - b * sin, b * cos + a * sin], -1).astype(jnp.bfloat16)


def seen_by(q, k, v):
    tokens, kv = q.shape[0], k.shape[1]
    q = q.reshape(tokens, kv, -1, q.shape[-1])
    scores = jnp.einsum("tgsd,ugd->gstu", q.astype(jnp.float32), k.astype(jnp.float32)) * q.shape[-1] ** -0.5
    place = jnp.arange(tokens)
    weights = jax.nn.softmax(jnp.where(place[:, None] >= place, scores, -jnp.inf), -1).astype(jnp.bfloat16)
    return jnp.einsum("gstu,ugd->tgsd", weights.astype(jnp.float32), v.astype(jnp.float32)).astype(jnp.bfloat16).reshape(tokens, -1)


def layer(h, w):
    a = normed(h)
    q, k = (turned(matmul(a, w[name]).reshape(h.shape[0], -1, HEAD), THETA) for name in ("wq", "wk"))
    h = h + matmul(seen_by(q, k, matmul(a, w["wv"]).reshape(h.shape[0], -1, HEAD)), w["wo"])
    b = normed(h)
    gate = jnp.dot(b, w["w_gate"], preferred_element_type=jnp.float32)
    up = jnp.dot(b, w["w_up"], preferred_element_type=jnp.float32)
    return h + matmul((jax.nn.silu(gate) * up).astype(jnp.bfloat16), w["w_down"])


def adamw(w, m, v, g):
    m = 0.9 * m + 0.1 * g
    v = 0.95 * v + 0.05 * g * g
    step = m * lax.rsqrt(v + 1e-8) + 0.1 * w
    return (w - 0.02 * step).astype(jnp.bfloat16), m, v


def clipped(gradients, sum_of_squares, count):
    factor = jnp.minimum(1.0, 0.5 * lax.rsqrt(sum_of_squares / count + 1e-30))
    return [g * factor for g in gradients]


def stack(weights, h):
    return lax.scan(lambda h, w: (layer(h, w), None), h, weights)[0]


def reference(x, dy, wq, wk, wv, wo, w_gate, w_up, w_down, m_wq, m_wk, m_wv, m_wo, m_w_gate, m_w_up, m_w_down, v_wq, v_wk, v_wv, v_wo, v_w_gate, v_w_up, v_w_down):
    weights = dict(zip(NAMES, (wq, wk, wv, wo, w_gate, w_up, w_down), strict=True))

    def take(so_far, sequence):
        h, by_y = sequence
        _, back = jax.vjp(stack, weights, h)
        by_weights, by_h = back(by_y)
        return jax.tree.map(lambda total, term: total + term.astype(jnp.float32), so_far, by_weights), by_h

    none_yet = {name: jnp.zeros(w.shape, jnp.float32) for name, w in weights.items()}
    by_weights, by_x = lax.scan(take, none_yet, (x, dy))
    gradients = [by_weights[name].astype(jnp.bfloat16).astype(jnp.float32) for name in NAMES]
    gradients = clipped(gradients, sum(jnp.sum(g * g) for g in gradients), sum(g.size for g in gradients))
    first = (m_wq, m_wk, m_wv, m_wo, m_w_gate, m_w_up, m_w_down)
    second = (v_wq, v_wk, v_wv, v_wo, v_w_gate, v_w_up, v_w_down)
    new = [adamw(weights[name].astype(jnp.float32), m, v, g) for name, m, v, g in zip(NAMES, first, second, gradients, strict=True)]
    return tuple(one[which] for which in range(3) for one in new)
```

```python
import functools

import jax
import jax.numpy as jnp
from jax import lax
from jax.experimental import pallas as pl
from jax.experimental.pallas import tpu as pltpu
from jax.sharding import PartitionSpec as P


NEG = -1e30
HIDDEN = 2 * NEG
LOG2E = 1.4426950408889634
VMEM = 58 * 2**20
STRIP = 512
HEAD = 128
THETA = 10000
EPS = 1e-6
BF, F32 = jnp.bfloat16, jnp.float32
ALL = ...


def _mm(a, b):
    return jnp.dot(a, b, preferred_element_type=F32)


def _by_rows(a, b):
    return lax.dot_general(a, b, (((1,), (1,)), ((), ())), preferred_element_type=F32)


def _params(*semantics):
    return pltpu.CompilerParams(dimension_semantics=semantics, vmem_limit_bytes=VMEM)


def _cost(flops, *arrays):
    return pl.CostEstimate(flops=int(flops), transcendentals=0, bytes_accessed=sum(a.size * a.dtype.itemsize for a in arrays))


def _norm(h_ref):
    wide = h_ref.astype(F32)
    scale = lax.rsqrt(jnp.mean(wide * wide, -1, keepdims=True) + EPS)
    return wide, scale, (wide * scale).astype(BF)


def _norm_bwd(wide, scale, by_normed):
    mean = jnp.mean(by_normed * wide, -1, keepdims=True)
    return by_normed * scale - wide * (scale * scale * scale * mean)


def _turn(t, cos, sin):
    heads = [t[:, a : a + HEAD] for a in range(0, t.shape[1], HEAD)]
    return jnp.concatenate([u * cos + pltpu.roll(u, HEAD // 2, 1) * sin for u in heads], 1)


def _qkv_kernel(h_ref, cos_ref, sin_ref, wq_ref, wk_ref, wv_ref, q_ref, k_ref, v_ref):
    a = _norm(h_ref[ALL])[2]
    cos, sin = cos_ref[ALL], sin_ref[ALL]
    q_ref[ALL] = _turn(_mm(a, wq_ref[ALL]).astype(BF).astype(F32), cos, sin).astype(BF)
    k_ref[ALL] = _turn(_mm(a, wk_ref[ALL]).astype(BF).astype(F32), cos, sin).astype(BF)
    v_ref[ALL] = _mm(a, wv_ref[ALL]).astype(BF)


def _of_layer(w, number):
    return pl.BlockSpec((None,) + w.shape[1:], lambda i: (number, 0, 0), pipeline_mode=pl.Buffered(1))


def _rows(bt, width):
    return pl.BlockSpec((bt, width), lambda i: (i, 0))


def _all(shape):
    return pl.BlockSpec(shape, lambda i: (0,) * len(shape))


def qkv(h, cos, sin, wq, wk, wv, number, bt=512):
    t, d = h.shape
    return pl.pallas_call(
        _qkv_kernel,
        grid=(t // bt,),
        in_specs=[_rows(bt, d), _rows(bt, HEAD), _rows(bt, HEAD)] + [_of_layer(w, number) for w in (wq, wk, wv)],
        out_specs=[_rows(bt, d)] * 3,
        out_shape=[jax.ShapeDtypeStruct((t, d), BF)] * 3,
        compiler_params=_params("parallel"),
        cost_estimate=_cost(6 * t * d * d, h, h, h, h, wq),
        name="qkv",
    )(h, cos, sin, wq, wk, wv)


def _gap(bk, bq):
    return lax.broadcasted_iota(jnp.int32, (bk, bq), 1) - lax.broadcasted_iota(jnp.int32, (bk, bq), 0)


def _attend_kernel(q_ref, k_ref, v_ref, o_ref, lse_ref, top_s, mix_s, gap_s, *, heads, scale, bq, bk):
    iq = pl.program_id(0)
    e = scale * LOG2E
    wide = min(bq, STRIP)
    pieces = [(i, at) for i in range(heads) for at in range(0, bq, wide)]

    @pl.when(iq == 0)
    def _():
        gap_s[ALL] = _gap(bk, bq)

    top_s[ALL] = jnp.full(top_s.shape, NEG, F32)
    mix_s[ALL] = jnp.zeros(mix_s.shape, F32)
    ones = jnp.ones((8, bk), BF)

    def block(j, masked):
        here = pl.ds(pl.multiple_of(j * bk, bk), bk)
        scores = [_by_rows(k_ref[here, i * HEAD : (i + 1) * HEAD], q_ref[at : at + wide, i * HEAD : (i + 1) * HEAD]) for i, at in pieces]
        ok = gap_s[ALL] >= j * bk - iq * bq if masked else None
        weights, keeps = [], []
        for (i, at), s in zip(pieces, scores):
            if masked:
                s = jnp.where(ok[:, at : at + wide], s, HIDDEN)
            old = top_s[i : i + 1, at : at + wide]
            top = jnp.maximum(old, s.max(axis=0, keepdims=True))
            top_s[i : i + 1, at : at + wide] = top
            weights.append(jnp.exp2((s - top) * e).astype(BF))
            keeps.append(jnp.exp2((old - top) * e))
        for (i, at), p, keep in zip(pieces, weights, keeps):
            values = jnp.concatenate([v_ref[here, i * HEAD : (i + 1) * HEAD].T, ones], axis=0)
            mix_s[i, :, at : at + wide] = mix_s[i, :, at : at + wide] * keep + _mm(values, p)

    whole = lax.div(iq * bq + 1, bk)
    last = lax.div(iq * bq + bq - 1 + bk, bk)
    lax.fori_loop(0, whole, lambda j, _: block(j, False), None)
    lax.fori_loop(whole, last, lambda j, _: block(j, True), None)

    for i in range(heads):
        total = mix_s[i, HEAD : HEAD + 1, :]
        o_ref[:, i * HEAD : (i + 1) * HEAD] = (mix_s[i, :HEAD, :] * (1 / total)).T.astype(BF)
        lse_ref[i : i + 1, :] = top_s[i : i + 1, :] * scale + jnp.log(total)


def attend(q, k, v, bq=1024, bk=512):
    t, d = q.shape
    heads = d // HEAD
    return pl.pallas_call(
        functools.partial(_attend_kernel, heads=heads, scale=HEAD**-0.5, bq=bq, bk=bk),
        grid=(t // bq,),
        in_specs=[_rows(bq, d), _all((t, d)), _all((t, d))],
        out_specs=[_rows(bq, d), pl.BlockSpec((heads, bq), lambda i: (0, i))],
        out_shape=[jax.ShapeDtypeStruct((t, d), BF), jax.ShapeDtypeStruct((heads, t), F32)],
        scratch_shapes=[pltpu.VMEM((heads, bq), F32), pltpu.VMEM((heads, HEAD + 8, bq), F32), pltpu.VMEM((bk, bq), jnp.int32)],
        compiler_params=_params("arbitrary"),
        cost_estimate=_cost(4 * t * t * d, q, k, v, q),
        name="attend",
    )(q, k, v)


def _attend_bwd_kernel(q_ref, k_ref, v_ref, do_ref, lse_ref, delta_ref, dq_ref, dk_ref, dv_ref, dq_s, dk_s, dv_s, gap_s, *, heads, scale, bq, bk):
    iq = pl.program_id(0)
    e = scale * LOG2E
    cols = [slice(i * HEAD, (i + 1) * HEAD) for i in range(heads)]

    @pl.when(iq == 0)
    def _():
        gap_s[ALL] = _gap(bk, bq)
        dk_s[ALL] = jnp.zeros_like(dk_s)
        dv_s[ALL] = jnp.zeros_like(dv_s)

    dq_s[ALL] = jnp.zeros_like(dq_s)

    def block(j, masked):
        here = pl.ds(pl.multiple_of(j * bk, bk), bk)
        scores = [_by_rows(k_ref[here, c], q_ref[:, c]) for c in cols]
        dps = [_by_rows(v_ref[here, c], do_ref[:, c]) for c in cols]
        ok = gap_s[ALL] >= j * bk - iq * bq if masked else None
        for i, c in enumerate(cols):
            p = jnp.exp2(scores[i] * e - lse_ref[i : i + 1, :] * LOG2E)
            if masked:
                p = jnp.where(ok, p, 0.0)
            ds = (p * (dps[i] - delta_ref[i : i + 1, :])).astype(BF)
            dv_s[i, here, :] += _mm(p.astype(BF), do_ref[:, c])
            dk_s[i, here, :] += _mm(ds, q_ref[:, c])
            dq_s[i] += _mm(k_ref[here, c].T, ds)

    whole = lax.div(iq * bq + 1, bk)
    last = lax.div(iq * bq + bq - 1 + bk, bk)
    lax.fori_loop(0, whole, lambda j, _: block(j, False), None)
    lax.fori_loop(whole, last, lambda j, _: block(j, True), None)
    for i, c in enumerate(cols):
        dq_ref[:, c] = (dq_s[i] * scale).T.astype(BF)

    @pl.when(iq == pl.num_programs(0) - 1)
    def _():
        for i, c in enumerate(cols):
            dk_ref[:, c] = (dk_s[i] * scale).astype(BF)
            dv_ref[:, c] = dv_s[i].astype(BF)


def attend_bwd(q, k, v, do, lse, delta, bq=512, bk=512):
    t, d = q.shape
    heads = d // HEAD
    stats = lambda a: pl.BlockSpec((a.shape[0], bq), lambda i: (0, i))
    return pl.pallas_call(
        functools.partial(_attend_bwd_kernel, heads=heads, scale=HEAD**-0.5, bq=bq, bk=bk),
        grid=(t // bq,),
        in_specs=[_rows(bq, d), _all((t, d)), _all((t, d)), _rows(bq, d), stats(lse), stats(delta)],
        out_specs=[_rows(bq, d), _all((t, d)), _all((t, d))],
        out_shape=[jax.ShapeDtypeStruct((t, d), BF)] * 3,
        scratch_shapes=[pltpu.VMEM((heads, HEAD, bq), F32), pltpu.VMEM((heads, t, HEAD), F32), pltpu.VMEM((heads, t, HEAD), F32),
                        pltpu.VMEM((bk, bq), jnp.int32)],
        compiler_params=_params("arbitrary"),
        cost_estimate=_cost(10 * t * t * d, q, k, v, do, q, k, v),
        name="attend_bwd",
    )(q, k, v, do, lse, delta)


FC = 512


def _hidden(b, wg_ref, wu_ref, at):
    gate = _mm(b, wg_ref[:, at])
    up = _mm(b, wu_ref[:, at])
    sig = jax.nn.sigmoid(gate)
    return gate, up, sig, gate * sig


def _ffn_kernel(h_ref, o_ref, wo_ref, wg_ref, wu_ref, wd_ref, h2_ref, h3_ref, y_s):
    h2 = (h_ref[ALL].astype(F32) + _mm(o_ref[ALL], wo_ref[ALL]).astype(BF).astype(F32)).astype(BF)
    h2_ref[ALL] = h2
    b = _norm(h2)[2]
    y_s[ALL] = jnp.zeros_like(y_s)

    def piece(j, _):
        at = pl.ds(pl.multiple_of(j * FC, FC), FC)
        _, up, _, act = _hidden(b, wg_ref, wu_ref, at)
        y_s[ALL] += _mm((act * up).astype(BF), wd_ref[at, :])

    lax.fori_loop(0, wg_ref.shape[-1] // FC, piece, None)
    h3_ref[ALL] = (h2.astype(F32) + y_s[ALL].astype(BF).astype(F32)).astype(BF)


def ffn(h, o, wo, wg, wu, wd, number, bt=512):
    t, d = h.shape
    return pl.pallas_call(
        _ffn_kernel,
        grid=(t // bt,),
        in_specs=[_rows(bt, d), _rows(bt, d)] + [_of_layer(w, number) for w in (wo, wg, wu, wd)],
        out_specs=[_rows(bt, d)] * 2,
        out_shape=[jax.ShapeDtypeStruct((t, d), BF)] * 2,
        scratch_shapes=[pltpu.VMEM((bt, d), F32)],
        compiler_params=_params("parallel"),
        cost_estimate=_cost(2 * t * d * (d + 3 * wg.shape[2]), h, o, h, h, wg, wg),
        name="ffn",
    )(h, o, wo, wg, wu, wd)


def _ffn_bwd_kernel(h_ref, o_ref, dy_ref, wo_ref, wg_ref, wu_ref, wd_ref, dh_ref, do_ref, delta_ref, grad_ref, dwo_ref, db_s, acc_s, acc_o, *, projected):
    i, steps = pl.program_id(0), pl.num_programs(0)
    d = h_ref.shape[1]
    n = wg_ref.shape[-1] // FC

    @pl.when(i == 0)
    def _():
        acc_s[ALL] = jnp.zeros_like(acc_s)
        acc_o[ALL] = jnp.zeros_like(acc_o)

    h2 = h_ref[ALL]
    if not projected:
        h2 = (h2.astype(F32) + _mm(o_ref[ALL], wo_ref[ALL]).astype(BF).astype(F32)).astype(BF)
    wide, scale, b = _norm(h2)
    dy = dy_ref[ALL]
    b_t, dy_t = b.T, dy.T
    db_s[ALL] = jnp.zeros_like(db_s)

    def piece(j, _):
        at = pl.ds(pl.multiple_of(j * FC, FC), FC)
        gate, up, sig, act = _hidden(b, wg_ref, wu_ref, at)
        u = (act * up).astype(BF)
        du = _by_rows(dy, wd_ref[at, :]).astype(BF).astype(F32)
        dup = (du * act).astype(BF)
        dgate = (du * up * (sig * (1 + gate * (1 - sig)))).astype(BF)
        acc_s[j] += _mm(b_t, dgate)
        acc_s[n + j] += _mm(b_t, dup)
        acc_s[2 * n + j] += _mm(dy_t, u)
        db_s[ALL] += _by_rows(dgate, wg_ref[:, at]) + _by_rows(dup, wu_ref[:, at])

    lax.fori_loop(0, n, piece, None)
    back = _norm_bwd(wide, scale, db_s[ALL].astype(BF).astype(F32)).astype(BF)
    dh = (dy.astype(F32) + back.astype(F32)).astype(BF)
    dh_ref[ALL] = dh
    do = _by_rows(dh, wo_ref[ALL]).astype(BF)
    do_ref[ALL] = do
    o = o_ref[ALL]
    acc_o[ALL] += _mm(o.T, dh)
    both = do.astype(F32) * o.astype(F32)
    lane = lax.broadcasted_iota(jnp.int32, (both.shape[0], HEAD), 1)
    delta = jnp.zeros((both.shape[0], HEAD), F32)
    for k in range(d // HEAD):
        delta = jnp.where(lane == k, jnp.sum(both[:, k * HEAD : (k + 1) * HEAD], 1, keepdims=True), delta)
    delta_ref[ALL] = delta.T[: delta_ref.shape[0], :]

    @pl.when(i == steps - 1)
    def _():
        def out(j, _):
            grad_ref[j] = acc_s[j].astype(BF)
            grad_ref[n + j] = acc_s[n + j].astype(BF)
            grad_ref[2 * n + j] = acc_s[2 * n + j].astype(BF).T

        lax.fori_loop(0, n, out, None)
        dwo_ref[ALL] = acc_o[ALL].astype(BF)


def ffn_bwd(h, o, dy, wo, wg, wu, wd, number, projected, bt=512):
    t, d = h.shape
    f = wg.shape[2]
    blocks = 3 * f // FC
    every = blocks + 4
    return pl.pallas_call(
        functools.partial(_ffn_bwd_kernel, projected=projected),
        grid=(t // bt,),
        in_specs=[_rows(bt, d)] * 3 + [_of_layer(w, number) for w in (wo, wg, wu, wd)],
        out_specs=[_rows(bt, d), _rows(bt, d), pl.BlockSpec((8, bt), lambda i: (0, i)), _all((blocks, d, FC)), _all((d, d))],
        out_shape=[jax.ShapeDtypeStruct((t, d), BF), jax.ShapeDtypeStruct((t, d), BF), jax.ShapeDtypeStruct((8, t), F32),
                   jax.ShapeDtypeStruct((every, d, FC), BF), jax.ShapeDtypeStruct((d, d), BF)],
        scratch_shapes=[pltpu.VMEM((bt, d), F32), pltpu.VMEM((blocks, d, FC), F32), pltpu.VMEM((d, d), F32)],
        compiler_params=_params("arbitrary"),
        cost_estimate=_cost(16 * t * d * f + 6 * t * d * d, h, o, dy, h, h, wg, wg, wg, wg),
        name="ffn_bwd",
    )(h, o, dy, wo, wg, wu, wd)


def _qkv_bwd_kernel(h_ref, dh2_ref, cos_ref, sin_ref, dq_ref, dk_ref, dv_ref, dwo_ref, wq_ref, wk_ref, wv_ref, _, *rest, needs_dh):
    dh_ref, (grad_ref, acc_s) = (rest[0], rest[1:]) if needs_dh else (None, rest)
    i, steps = pl.program_id(0), pl.num_programs(0)

    @pl.when(i == 0)
    def _():
        acc_s[ALL] = jnp.zeros_like(acc_s)

    wide, scale, a = _norm(h_ref[ALL])
    cos, sin = cos_ref[ALL], -sin_ref[ALL]
    dq = _turn(dq_ref[ALL].astype(F32), cos, sin).astype(BF)
    dk = _turn(dk_ref[ALL].astype(F32), cos, sin).astype(BF)
    dv = dv_ref[ALL]
    a_t = a.T
    acc_s[0] += _mm(a_t, dq)
    acc_s[1] += _mm(a_t, dk)
    acc_s[2] += _mm(a_t, dv)
    if needs_dh:
        da = _by_rows(dq, wq_ref[ALL]) + _by_rows(dk, wk_ref[ALL]) + _by_rows(dv, wv_ref[ALL])
        back = _norm_bwd(wide, scale, da.astype(BF).astype(F32)).astype(BF)
        dh_ref[ALL] = (dh2_ref[ALL].astype(F32) + back.astype(F32)).astype(BF)

    @pl.when(i == steps - 1)
    def _():
        for k in range(3):
            grad_ref[k] = acc_s[k].astype(BF)
        grad_ref[3] = dwo_ref[ALL]


def qkv_bwd(h, dh2, cos, sin, dq, dk, dv, dwo, wq, wk, wv, grads, number, needs_dh, bt=512):
    t, d = h.shape
    last = grads.shape[0] // 4 - 1
    got = pl.pallas_call(
        functools.partial(_qkv_bwd_kernel, needs_dh=needs_dh),
        grid=(t // bt,),
        in_specs=[_rows(bt, d), _rows(bt, d), _rows(bt, HEAD), _rows(bt, HEAD)] + [_rows(bt, d)] * 3 + [_all((d, d))]
        + [_of_layer(w, number) for w in (wq, wk, wv)] + [pl.BlockSpec(memory_space=pl.ANY)],
        out_specs=[_rows(bt, d)] * needs_dh + [pl.BlockSpec((4, d, d), lambda i: (last, 0, 0))],
        out_shape=[jax.ShapeDtypeStruct((t, d), BF)] * needs_dh + [jax.ShapeDtypeStruct(grads.shape, BF)],
        input_output_aliases={11: int(needs_dh)},
        scratch_shapes=[pltpu.VMEM((3, d, d), F32)],
        compiler_params=_params("arbitrary"),
        cost_estimate=_cost((6 + 6 * needs_dh) * t * d * d, h, h, h, h, h, h, wq),
        name="qkv_bwd",
    )(h, dh2, cos, sin, dq, dk, dv, dwo, wq, wk, wv, grads)
    return got if needs_dh else (None, *got)


STEPS = 16


def _adamw_kernel(f_ref, *refs):
    factor = f_ref[0, 0]
    grads, ins, outs = refs[:4], refs[4:25], refs[-21:]
    for n in range(7):
        (w_ref, m_ref, v_ref), (nw_ref, nm_ref, nv_ref) = ins[n::7], outs[n::7]
        g = (grads[3][n] if n < 4 else grads[n - 4][ALL]).astype(F32) * factor
        m = 0.9 * m_ref[ALL] + 0.1 * g
        v = 0.95 * v_ref[ALL] + 0.05 * g * g
        w = w_ref[ALL].astype(F32)
        nw_ref[ALL] = (w - 0.02 * (m * lax.rsqrt(v + 1e-8) + 0.1 * w)).astype(BF)
        nm_ref[ALL] = m
        nv_ref[ALL] = v


def adamw(factor, grads, arrays, layer, into):
    d = arrays[0].shape[1]
    per = arrays[4].shape[2] // FC
    cut = STEPS // per
    rows, few = d // cut, d // STEPS
    wide = lambda n: pl.BlockSpec((None, rows, FC), lambda j: (n * per + j // cut, j % cut, 0))
    blocks = [wide(0), wide(1), wide(2), pl.BlockSpec((4, few, FC), lambda j: (3 * per // 4, j, 0))]
    small = pl.BlockSpec((None, few, d), lambda j: (layer, j, 0))
    across = pl.BlockSpec((None, rows, FC), lambda j: (layer, j % cut, j // cut))
    down = pl.BlockSpec((None, rows, FC), lambda j: (layer, j, 0))
    specs = ([small] * 4 + [across] * 2 + [down]) * 3
    first = 1 + len(blocks) + len(arrays)
    return pl.pallas_call(
        _adamw_kernel,
        grid=(STEPS,),
        in_specs=[pl.BlockSpec(memory_space=pltpu.SMEM)] + blocks + specs + [pl.BlockSpec(memory_space=pl.ANY)] * len(into),
        out_specs=specs,
        out_shape=[jax.ShapeDtypeStruct(a.shape, a.dtype) for a in arrays],
        input_output_aliases={first + n: n for n in range(len(into))},
        compiler_params=_params("arbitrary"),
        cost_estimate=_cost(10**10, *arrays),
        name="adamw",
    )(factor, *[grads] * 4, *arrays, *into)


ZS = 4
GROUP = 32
PARTS = 2


def _coords():
    i = lax.axis_index("dp")
    return i // 16, i // 8 % 2, i // 2 % 4, i % 2


def _number(x, y, z, c):
    return ((x * 2 + y) * ZS + z) * 2 + c


def _copy(src, dst, send, recv, to):
    return pltpu.make_async_remote_copy(src_ref=src, dst_ref=dst, send_sem=send, recv_sem=recv, device_id={"dp": to},
                                        device_id_type=pl.DeviceIdType.MESH)


def _add(out, *terms):
    step = 32

    def some(k, _):
        at = pl.ds(pl.multiple_of(k * step, step), step)
        total = terms[0][at, :].astype(F32)
        for t in terms[1:]:
            total += t[at, :].astype(F32)
        out[at, :] = total.astype(BF)

    lax.fori_loop(0, out.shape[0] // step, some, None)


class _Scatter:
    @staticmethod
    def scratch(rows, n):
        b = rows // 16
        sem = pltpu.SemaphoreType.DMA
        return [pltpu.VMEM((8, b, n), BF), pltpu.VMEM((8, b, n), BF), pltpu.VMEM((4, b, n), BF), pltpu.VMEM((2, b, n), BF),
                pltpu.VMEM((6, b // ZS, n), BF), sem((8,)), sem((8,)), sem((8,)), sem((4,)), sem((4,)), sem((2,)), sem((2,)), sem((6,)), sem((6,))]

    def __init__(self, g_ref, share_ref, refs):
        (self.own, self.rc, self.ra, self.rb, self.rz, local, cs, cr, as_, ar, bs, br, zs, zr) = refs
        self.share = share_ref
        x, y, z, c = _coords()
        self.z, self.r = z, g_ref.shape[0] // 64
        b = ZS * self.r
        peer = {"x": _number(1 - x, y, z, c), "y": _number(x, 1 - y, z, c), "c": _number(x, y, z, 1 - c)}
        place = lambda c, h, x, y: g_ref.at[pl.ds(pl.multiple_of((((c * 2 + h) * 2 + x) * 2 + y) * b, b), b)]
        self.local, self.core = [], []
        for n in range(8):
            h, first, second = n // 4, n // 2 % 2, n % 2
            dx, dy = (first, second) if h == 0 else (second, first)
            bx, by = (x + dx) % 2, (y + dy) % 2
            self.local.append(pltpu.make_async_copy(place(c, h, bx, by), self.own.at[n], local.at[n]))
            self.core.append(_copy(place(1 - c, h, bx, by), self.rc.at[n], cs.at[n], cr.at[n], peer["c"]))
        axes = ("xy", "yx")
        self.a = [_copy(self.own.at[h * 4 + 2 + s], self.ra.at[h * 2 + s], as_.at[h * 2 + s], ar.at[h * 2 + s], peer[axes[h][0]])
                  for h in range(2) for s in range(2)]
        self.b = [_copy(self.own.at[h * 4 + 1], self.rb.at[h], bs.at[h], br.at[h], peer[axes[h][1]]) for h in range(2)]
        self.zc = []
        for h in range(2):
            for k in (1, 2, 3):
                to = (z + k) % ZS
                n = h * 3 + k - 1
                self.zc.append(_copy(self.own.at[h * 4, pl.ds(pl.multiple_of(to * self.r, self.r), self.r)], self.rz.at[n], zs.at[n], zr.at[n],
                                     _number(x, y, to, c)))

    def start(self):
        for n in (2, 6, 3, 7, 1, 5, 0, 4):
            self.core[n].start()
            self.local[n].start()

    def _core(self, n):
        self.core[n].wait_recv()
        self.local[n].wait()
        _add(self.own.at[n], self.own.at[n], self.rc.at[n])

    def first(self):
        for s in (1, 0):
            for h in (0, 1):
                self._core(h * 4 + 2 + s)
                self.a[h * 2 + s].start()

    def keep(self):
        for n in (1, 5, 0, 4):
            self._core(n)

    def second(self):
        for h in (0, 1):
            self.a[h * 2 + 1].wait_recv()
            _add(self.own.at[h * 4 + 1], self.own.at[h * 4 + 1], self.ra.at[h * 2 + 1])
            self.b[h].start()

    def third(self):
        for h in (0, 1):
            self.a[h * 2].wait_recv()
            self.b[h].wait_recv()
            mine = self.own.at[h * 4]
            _add(mine, mine, self.ra.at[h * 2], self.rb.at[h])
            for k in (0, 1, 2):
                self.zc[h * 3 + k].start()

    def last(self):
        for h in (0, 1):
            for k in (0, 1, 2):
                self.zc[h * 3 + k].wait_recv()
            mine = self.own.at[h * 4, pl.ds(pl.multiple_of(self.z * self.r, self.r), self.r)]
            _add(self.share.at[pl.ds(h * self.r, self.r)], mine, *[self.rz.at[h * 3 + k] for k in (0, 1, 2)])
        for copy in self.core + self.a + self.b + self.zc:
            copy.wait_send()

    def phases(self):
        return [self.start, self.first, self.keep, self.second, self.third, self.last]


def _scatter_kernel(g_ref, s_ref, *refs):
    per = len(_Scatter.scratch(1024, HEAD))
    rows, own = g_ref.shape[0] // PARTS, s_ref.shape[0] // PARTS
    part = [_Scatter(g_ref.at[pl.ds(k * rows, rows)], s_ref.at[pl.ds(k * own, own)], refs[k * per : (k + 1) * per]) for k in range(PARTS)]
    for p in part:
        p.start()
    for t in range(PARTS + 2):
        if t < PARTS:
            part[t].first()
        if 0 <= t - 1 < PARTS:
            part[t - 1].keep()
            part[t - 1].second()
        if 0 <= t - 2 < PARTS:
            part[t - 2].third()
    for p in part:
        p.last()


def scattered_sum(g):
    rows, n = g.shape
    return pl.pallas_call(
        _scatter_kernel,
        in_specs=[pl.BlockSpec(memory_space=pl.ANY)],
        out_specs=pl.BlockSpec(memory_space=pltpu.VMEM),
        out_shape=jax.ShapeDtypeStruct((rows // GROUP, n), BF),
        scratch_shapes=_Scatter.scratch(rows // PARTS, n) * PARTS,
        compiler_params=pltpu.CompilerParams(vmem_limit_bytes=VMEM, has_side_effects=True),
        cost_estimate=pl.CostEstimate(flops=10**10, transcendentals=0, bytes_accessed=10**7),
        name="scatter",
    )(g)


class _Gather:
    @staticmethod
    def scratch():
        sem = pltpu.SemaphoreType.DMA
        return [sem((2,)), sem((6,)), sem((6,)), sem((8,)), sem((8,)), sem((16,)), sem((16,)), sem((32,)), sem((32,))]

    def __init__(self, share_ref, out_ref, refs):
        local, zs, zr, ss, sr, ts, tr, cs, cr = refs
        x, y, z, c = _coords()
        r = share_ref.shape[0] // 2
        where = lambda h, x, y, z: out_ref.at[pl.ds(pl.multiple_of(((((c * 2 + h) * 2 + x) * 2 + y) * ZS + z) * r, r), r)]
        to_x, to_y, to_c = _number(1 - x, y, z, c), _number(x, 1 - y, z, c), _number(x, y, z, 1 - c)
        self.local, self.z, self.s, self.t, self.c = [], {}, {}, {}, {}
        for h in range(2):
            own = share_ref.at[pl.ds(h * r, r)]
            self.local.append(pltpu.make_async_copy(own, where(h, x, y, z), local.at[h]))
            for k in (1, 2, 3):
                n = h * 3 + k - 1
                self.z[h, k] = _copy(own, where(h, x, y, z), zs.at[n], zr.at[n], _number(x, y, (z + k) % ZS, c))
            for k in range(4):
                bz = (z + ZS - k) % ZS
                near = where(h, x, y, bz)
                src = own if k == 0 else near
                n = h * 4 + k
                self.s[h, k] = _copy(src, near, ss.at[n], sr.at[n], (to_y, to_x)[h])
                for side in range(2):
                    far = near if side == 0 else (where(0, x, 1 - y, bz), where(1, 1 - x, y, bz))[h]
                    n = (h * 4 + k) * 2 + side
                    self.t[h, k, side] = _copy(src if side == 0 else far, far, ts.at[n], tr.at[n], (to_x, to_y)[h])
                for side in range(4):
                    at = where(h, (x, x, 1 - x, 1 - x)[side] if h == 0 else (x, 1 - x, x, 1 - x)[side],
                               (y, 1 - y, y, 1 - y)[side] if h == 0 else (y, y, 1 - y, 1 - y)[side], bz)
                    n = (h * 4 + k) * 4 + side
                    self.c[h, k, side] = _copy(src if side == 0 else at, at, cs.at[n], cr.at[n], to_c)

    def _near(self, h, k):
        self.s[h, k].start()
        self.t[h, k, 0].start()
        self.c[h, k, 0].start()

    def start(self):
        for h in (0, 1):
            self.local[h].start()
            for k in (2, 1, 3):
                self.z[h, k].start()
            self._near(h, 0)

    def first(self):
        for k in (2, 1, 3):
            for h in (0, 1):
                self.z[h, k].wait_recv()
                self._near(h, k)

    def second(self):
        for k in (0, 2, 1, 3):
            for h in (0, 1):
                self.s[h, k].wait_recv()
                self.t[h, k, 1].start()
                self.c[h, k, 1].start()

    def third(self):
        for side in (0, 1):
            for k in (0, 2, 1, 3):
                for h in (0, 1):
                    self.t[h, k, side].wait_recv()
                    self.c[h, k, 2 + side].start()

    def last(self):
        for copy in self.c.values():
            copy.wait_recv()
        for copies in (self.z, self.s, self.t, self.c):
            for copy in copies.values():
                copy.wait_send()
        for copy in self.local:
            copy.wait()

    def phases(self):
        return [self.start, self.first, self.second, self.third, self.last]


def _gather_kernel(s_ref, other_ref, g_ref, sum_ref, all_ref, send, recv, *refs):
    per = len(_Gather.scratch())
    rows, own = g_ref.shape[0] // PARTS, s_ref.shape[0] // PARTS
    part = [_Gather(s_ref.at[pl.ds(k * own, own)], g_ref.at[pl.ds(k * rows, rows)], refs[k * per : (k + 1) * per]) for k in range(PARTS)]
    for p in part:
        p.start()

    def squares(ref, total):
        def some(k, total):
            g = ref[pl.ds(pl.multiple_of(k * 8, 8), 8), :].astype(F32)
            g = g * g
            for at in range(0, ref.shape[1], HEAD):
                total = total + g[:, at : at + HEAD]
            return total

        return lax.fori_loop(0, ref.shape[0] // 8, some, total)

    me = lax.axis_index("dp")
    none = jnp.zeros(sum_ref.shape, F32)
    all_ref[me] = squares(other_ref, squares(s_ref, none))

    def told(k):
        return _copy(all_ref.at[me], all_ref.at[me], send.at[k], recv.at[k], (me + k) % GROUP)

    lax.fori_loop(1, GROUP, lambda k, _: told(k).start(), None)
    for p in part:
        p.first()
    for p in part:
        p.second()
    lax.fori_loop(1, GROUP, lambda k, _: told(k).wait_recv(), None)
    sum_ref[ALL] = lax.fori_loop(0, GROUP, lambda k, t: t + all_ref[k], none)
    for p in part:
        p.third()
    for p in part:
        p.last()
    lax.fori_loop(1, GROUP, lambda k, _: told(k).wait_send(), None)


def gathered(s, other):
    rows, n = s.shape
    vmem = pl.BlockSpec(memory_space=pltpu.VMEM)
    sem = pltpu.SemaphoreType.DMA((GROUP,))
    return pl.pallas_call(
        _gather_kernel,
        in_specs=[vmem, vmem],
        out_specs=[pl.BlockSpec(memory_space=pl.ANY), vmem],
        out_shape=[jax.ShapeDtypeStruct((rows * GROUP, n), BF), jax.ShapeDtypeStruct((8, HEAD), F32)],
        scratch_shapes=[pltpu.VMEM((GROUP, 8, HEAD), F32), sem, sem] + _Gather.scratch() * PARTS,
        compiler_params=pltpu.CompilerParams(vmem_limit_bytes=VMEM, has_side_effects=True),
        cost_estimate=pl.CostEstimate(flops=10**10, transcendentals=0, bytes_accessed=10**7),
        name="gather",
    )(s, other)


def solution(mesh):
    def step(x, dy, *arrays):
        weights = arrays[:7]
        wq, wk, wv, wo, wg, wu, wd = weights
        layers = wq.shape[0]
        h, dh = x[0], dy[0]
        half = HEAD // 2
        angle = jnp.arange(h.shape[0], dtype=F32)[:, None] * THETA ** (-jnp.arange(half, dtype=F32) / half)
        cos, sin = jnp.cos(angle), jnp.sin(angle)
        cos, sin = jnp.concatenate([cos, cos], 1), jnp.concatenate([-sin, sin], 1)
        kept = []
        for n in range(layers):
            q, k, val = qkv(h, cos, sin, wq, wk, wv, n)
            o, lse = attend(q, k, val)
            if n < layers - 1:
                h2, h3 = ffn(h, o, wo, wg, wu, wd, n)
            else:
                h2, h3 = h, None
            kept.append((h, q, k, val, o, lse, h2))
            h = h3
        grads = [None] * layers
        for n in reversed(range(layers)):
            h, q, k, val, o, lse, h2 = kept[n]
            dh2, do, delta, some, dwo = ffn_bwd(h2, o, dh, wo, wg, wu, wd, n, n < layers - 1)
            dq, dk, dval = attend_bwd(q, k, val, do, lse, delta)
            dh, grads[n] = qkv_bwd(h, dh2, cos, sin, dq, dk, dval, dwo, wq, wk, wv, some, n, n > 0)
            if n == 1:
                s1 = lax.psum_scatter(grads[1].reshape(-1, FC), "dp", scatter_dimension=0, tiled=True)
        shape = grads[0].shape
        s0 = scattered_sum(grads[0].reshape(-1, FC))
        g1 = lax.all_gather(s1, "dp", axis=0, tiled=True)
        g0, squares = gathered(s0, s1)
        count = sum(w.size for w in weights)
        factor = jnp.minimum(1.0, 0.5 * lax.rsqrt(jnp.sum(squares) / count + 1e-30)).reshape(1, 1)
        new = ()
        for n, g in enumerate((g0, g1)):
            new = adamw(factor, g.reshape(shape), arrays, n, new)
        return tuple(new)

    states, all_of = P(("rep", "dp"), None, None), P(None, None, None)
    return jax.shard_map(
        step,
        mesh=mesh,
        in_specs=(states, states) + (all_of,) * 21,
        out_specs=(P("rep", None, None),) * 21,
        check_vma=False,
    )
```

```python
import functools

import jax
import jax.numpy as jnp
from jax import lax
from jax.experimental import pallas as pl
from jax.experimental.pallas import tpu as pltpu
from jax.sharding import PartitionSpec as P


NEG = -1e30
HIDDEN = 2 * NEG
LOG2E = 1.4426950408889634
VMEM = 58 * 2**20
STRIP = 512
HEAD = 128
THETA = 10000
EPS = 1e-6
BF, F32 = jnp.bfloat16, jnp.float32
ALL = ...


def _mm(a, b):
    return jnp.dot(a, b, preferred_element_type=F32)


def _by_rows(a, b):
    return lax.dot_general(a, b, (((1,), (1,)), ((), ())), preferred_element_type=F32)


def _params(*semantics):
    return pltpu.CompilerParams(dimension_semantics=semantics, vmem_limit_bytes=VMEM)


def _cost(flops, *arrays):
    return pl.CostEstimate(flops=int(flops), transcendentals=0, bytes_accessed=sum(a.size * a.dtype.itemsize for a in arrays))


def _norm(h_ref):
    wide = h_ref.astype(F32)
    scale = lax.rsqrt(jnp.mean(wide * wide, -1, keepdims=True) + EPS)
    return wide, scale, (wide * scale).astype(BF)


def _norm_bwd(wide, scale, by_normed):
    mean = jnp.mean(by_normed * wide, -1, keepdims=True)
    return by_normed * scale - wide * (scale * scale * scale * mean)


def _turn(t, cos, sin):
    heads = [t[:, a : a + HEAD] for a in range(0, t.shape[1], HEAD)]
    return jnp.concatenate([u * cos + pltpu.roll(u, HEAD // 2, 1) * sin for u in heads], 1)


def _qkv_kernel(h_ref, cos_ref, sin_ref, wq_ref, wk_ref, wv_ref, q_ref, k_ref, v_ref):
    a = _norm(h_ref[ALL])[2]
    cos, sin = cos_ref[ALL], sin_ref[ALL]
    q_ref[ALL] = _turn(_mm(a, wq_ref[ALL]).astype(BF).astype(F32), cos, sin).astype(BF)
    k_ref[ALL] = _turn(_mm(a, wk_ref[ALL]).astype(BF).astype(F32), cos, sin).astype(BF)
    v_ref[ALL] = _mm(a, wv_ref[ALL]).astype(BF)


def _of_layer(w, number):
    return pl.BlockSpec((None,) + w.shape[1:], lambda i: (number, 0, 0), pipeline_mode=pl.Buffered(1))


def _rows(bt, width):
    return pl.BlockSpec((bt, width), lambda i: (i, 0))


def _all(shape):
    return pl.BlockSpec(shape, lambda i: (0,) * len(shape))


def qkv(h, cos, sin, wq, wk, wv, number, bt=512):
    t, d = h.shape
    return pl.pallas_call(
        _qkv_kernel,
        grid=(t // bt,),
        in_specs=[_rows(bt, d), _rows(bt, HEAD), _rows(bt, HEAD)] + [_of_layer(w, number) for w in (wq, wk, wv)],
        out_specs=[_rows(bt, d)] * 3,
        out_shape=[jax.ShapeDtypeStruct((t, d), BF)] * 3,
        compiler_params=_params("parallel"),
        cost_estimate=_cost(6 * t * d * d, h, h, h, h, wq),
        name="qkv",
    )(h, cos, sin, wq, wk, wv)


def _gap(bk, bq):
    return lax.broadcasted_iota(jnp.int32, (bk, bq), 1) - lax.broadcasted_iota(jnp.int32, (bk, bq), 0)


def _attend_kernel(q_ref, k_ref, v_ref, o_ref, lse_ref, top_s, mix_s, gap_s, *, heads, scale, bq, bk):
    iq = pl.program_id(0)
    e = scale * LOG2E
    wide = min(bq, STRIP)
    pieces = [(i, at) for i in range(heads) for at in range(0, bq, wide)]

    @pl.when(iq == 0)
    def _():
        gap_s[ALL] = _gap(bk, bq)

    top_s[ALL] = jnp.full(top_s.shape, NEG, F32)
    mix_s[ALL] = jnp.zeros(mix_s.shape, F32)
    ones = jnp.ones((8, bk), BF)

    def block(j, masked):
        here = pl.ds(pl.multiple_of(j * bk, bk), bk)
        scores = [_by_rows(k_ref[here, i * HEAD : (i + 1) * HEAD], q_ref[at : at + wide, i * HEAD : (i + 1) * HEAD]) for i, at in pieces]
        ok = gap_s[ALL] >= j * bk - iq * bq if masked else None
        weights, keeps = [], []
        for (i, at), s in zip(pieces, scores):
            if masked:
                s = jnp.where(ok[:, at : at + wide], s, HIDDEN)
            old = top_s[i : i + 1, at : at + wide]
            top = jnp.maximum(old, s.max(axis=0, keepdims=True))
            top_s[i : i + 1, at : at + wide] = top
            weights.append(jnp.exp2((s - top) * e).astype(BF))
            keeps.append(jnp.exp2((old - top) * e))
        for (i, at), p, keep in zip(pieces, weights, keeps):
            values = jnp.concatenate([v_ref[here, i * HEAD : (i + 1) * HEAD].T, ones], axis=0)
            mix_s[i, :, at : at + wide] = mix_s[i, :, at : at + wide] * keep + _mm(values, p)

    whole = lax.div(iq * bq + 1, bk)
    last = lax.div(iq * bq + bq - 1 + bk, bk)
    lax.fori_loop(0, whole, lambda j, _: block(j, False), None)
    lax.fori_loop(whole, last, lambda j, _: block(j, True), None)

    for i in range(heads):
        total = mix_s[i, HEAD : HEAD + 1, :]
        o_ref[:, i * HEAD : (i + 1) * HEAD] = (mix_s[i, :HEAD, :] * (1 / total)).T.astype(BF)
        lse_ref[i : i + 1, :] = top_s[i : i + 1, :] * scale + jnp.log(total)


def attend(q, k, v, bq=1024, bk=512):
    t, d = q.shape
    heads = d // HEAD
    return pl.pallas_call(
        functools.partial(_attend_kernel, heads=heads, scale=HEAD**-0.5, bq=bq, bk=bk),
        grid=(t // bq,),
        in_specs=[_rows(bq, d), _all((t, d)), _all((t, d))],
        out_specs=[_rows(bq, d), pl.BlockSpec((heads, bq), lambda i: (0, i))],
        out_shape=[jax.ShapeDtypeStruct((t, d), BF), jax.ShapeDtypeStruct((heads, t), F32)],
        scratch_shapes=[pltpu.VMEM((heads, bq), F32), pltpu.VMEM((heads, HEAD + 8, bq), F32), pltpu.VMEM((bk, bq), jnp.int32)],
        compiler_params=_params("arbitrary"),
        cost_estimate=_cost(4 * t * t * d, q, k, v, q),
        name="attend",
    )(q, k, v)


def _attend_bwd_kernel(q_ref, k_ref, v_ref, do_ref, lse_ref, delta_ref, dq_ref, dk_ref, dv_ref, dq_s, dk_s, dv_s, gap_s, *, heads, scale, bq, bk):
    iq = pl.program_id(0)
    e = scale * LOG2E
    cols = [slice(i * HEAD, (i + 1) * HEAD) for i in range(heads)]

    @pl.when(iq == 0)
    def _():
        gap_s[ALL] = _gap(bk, bq)
        dk_s[ALL] = jnp.zeros_like(dk_s)
        dv_s[ALL] = jnp.zeros_like(dv_s)

    dq_s[ALL] = jnp.zeros_like(dq_s)

    def block(j, masked):
        here = pl.ds(pl.multiple_of(j * bk, bk), bk)
        scores = [_by_rows(k_ref[here, c], q_ref[:, c]) for c in cols]
        dps = [_by_rows(v_ref[here, c], do_ref[:, c]) for c in cols]
        ok = gap_s[ALL] >= j * bk - iq * bq if masked else None
        for i, c in enumerate(cols):
            p = jnp.exp2(scores[i] * e - lse_ref[i : i + 1, :] * LOG2E)
            if masked:
                p = jnp.where(ok, p, 0.0)
            ds = (p * (dps[i] - delta_ref[i : i + 1, :])).astype(BF)
            dv_s[i, here, :] += _mm(p.astype(BF), do_ref[:, c])
            dk_s[i, here, :] += _mm(ds, q_ref[:, c])
            dq_s[i] += _mm(k_ref[here, c].T, ds)

    whole = lax.div(iq * bq + 1, bk)
    last = lax.div(iq * bq + bq - 1 + bk, bk)
    lax.fori_loop(0, whole, lambda j, _: block(j, False), None)
    lax.fori_loop(whole, last, lambda j, _: block(j, True), None)
    for i, c in enumerate(cols):
        dq_ref[:, c] = (dq_s[i] * scale).T.astype(BF)

    @pl.when(iq == pl.num_programs(0) - 1)
    def _():
        for i, c in enumerate(cols):
            dk_ref[:, c] = (dk_s[i] * scale).astype(BF)
            dv_ref[:, c] = dv_s[i].astype(BF)


def attend_bwd(q, k, v, do, lse, delta, bq=512, bk=512):
    t, d = q.shape
    heads = d // HEAD
    stats = lambda a: pl.BlockSpec((a.shape[0], bq), lambda i: (0, i))
    return pl.pallas_call(
        functools.partial(_attend_bwd_kernel, heads=heads, scale=HEAD**-0.5, bq=bq, bk=bk),
        grid=(t // bq,),
        in_specs=[_rows(bq, d), _all((t, d)), _all((t, d)), _rows(bq, d), stats(lse), stats(delta)],
        out_specs=[_rows(bq, d), _all((t, d)), _all((t, d))],
        out_shape=[jax.ShapeDtypeStruct((t, d), BF)] * 3,
        scratch_shapes=[pltpu.VMEM((heads, HEAD, bq), F32), pltpu.VMEM((heads, t, HEAD), F32), pltpu.VMEM((heads, t, HEAD), F32),
                        pltpu.VMEM((bk, bq), jnp.int32)],
        compiler_params=_params("arbitrary"),
        cost_estimate=_cost(10 * t * t * d, q, k, v, do, q, k, v),
        name="attend_bwd",
    )(q, k, v, do, lse, delta)


FC = 512


def _hidden(b, wg_ref, wu_ref, at):
    gate = _mm(b, wg_ref[:, at])
    up = _mm(b, wu_ref[:, at])
    sig = jax.nn.sigmoid(gate)
    return gate, up, sig, gate * sig


def _ffn_kernel(h_ref, o_ref, wo_ref, wg_ref, wu_ref, wd_ref, h2_ref, h3_ref, y_s):
    h2 = (h_ref[ALL].astype(F32) + _mm(o_ref[ALL], wo_ref[ALL]).astype(BF).astype(F32)).astype(BF)
    h2_ref[ALL] = h2
    b = _norm(h2)[2]
    y_s[ALL] = jnp.zeros_like(y_s)

    def piece(j, _):
        at = pl.ds(pl.multiple_of(j * FC, FC), FC)
        _, up, _, act = _hidden(b, wg_ref, wu_ref, at)
        y_s[ALL] += _mm((act * up).astype(BF), wd_ref[at, :])

    lax.fori_loop(0, wg_ref.shape[-1] // FC, piece, None)
    h3_ref[ALL] = (h2.astype(F32) + y_s[ALL].astype(BF).astype(F32)).astype(BF)


def ffn(h, o, wo, wg, wu, wd, number, bt=512):
    t, d = h.shape
    return pl.pallas_call(
        _ffn_kernel,
        grid=(t // bt,),
        in_specs=[_rows(bt, d), _rows(bt, d)] + [_of_layer(w, number) for w in (wo, wg, wu, wd)],
        out_specs=[_rows(bt, d)] * 2,
        out_shape=[jax.ShapeDtypeStruct((t, d), BF)] * 2,
        scratch_shapes=[pltpu.VMEM((bt, d), F32)],
        compiler_params=_params("parallel"),
        cost_estimate=_cost(2 * t * d * (d + 3 * wg.shape[2]), h, o, h, h, wg, wg),
        name="ffn",
    )(h, o, wo, wg, wu, wd)


def _ffn_bwd_kernel(h_ref, o_ref, dy_ref, wo_ref, wg_ref, wu_ref, wd_ref, dh_ref, do_ref, delta_ref, grad_ref, dwo_ref, db_s, acc_s, acc_o, *, projected):
    i, steps = pl.program_id(0), pl.num_programs(0)
    d = h_ref.shape[1]
    n = wg_ref.shape[-1] // FC

    @pl.when(i == 0)
    def _():
        acc_s[ALL] = jnp.zeros_like(acc_s)
        acc_o[ALL] = jnp.zeros_like(acc_o)

    h2 = h_ref[ALL]
    if not projected:
        h2 = (h2.astype(F32) + _mm(o_ref[ALL], wo_ref[ALL]).astype(BF).astype(F32)).astype(BF)
    wide, scale, b = _norm(h2)
    dy = dy_ref[ALL]
    b_t, dy_t = b.T, dy.T
    db_s[ALL] = jnp.zeros_like(db_s)

    def piece(j, _):
        at = pl.ds(pl.multiple_of(j * FC, FC), FC)
        gate, up, sig, act = _hidden(b, wg_ref, wu_ref, at)
        u = (act * up).astype(BF)
        du = _by_rows(dy, wd_ref[at, :]).astype(BF).astype(F32)
        dup = (du * act).astype(BF)
        dgate = (du * up * (sig * (1 + gate * (1 - sig)))).astype(BF)
        acc_s[j] += _mm(b_t, dgate)
        acc_s[n + j] += _mm(b_t, dup)
        acc_s[2 * n + j] += _mm(dy_t, u)
        db_s[ALL] += _by_rows(dgate, wg_ref[:, at]) + _by_rows(dup, wu_ref[:, at])

    lax.fori_loop(0, n, piece, None)
    back = _norm_bwd(wide, scale, db_s[ALL].astype(BF).astype(F32)).astype(BF)
    dh = (dy.astype(F32) + back.astype(F32)).astype(BF)
    dh_ref[ALL] = dh
    do = _by_rows(dh, wo_ref[ALL]).astype(BF)
    do_ref[ALL] = do
    o = o_ref[ALL]
    acc_o[ALL] += _mm(o.T, dh)
    both = do.astype(F32) * o.astype(F32)
    lane = lax.broadcasted_iota(jnp.int32, (both.shape[0], HEAD), 1)
    delta = jnp.zeros((both.shape[0], HEAD), F32)
    for k in range(d // HEAD):
        delta = jnp.where(lane == k, jnp.sum(both[:, k * HEAD : (k + 1) * HEAD], 1, keepdims=True), delta)
    delta_ref[ALL] = delta.T[: delta_ref.shape[0], :]

    @pl.when(i == steps - 1)
    def _():
        def out(j, _):
            grad_ref[j] = acc_s[j].astype(BF)
            grad_ref[n + j] = acc_s[n + j].astype(BF)
            grad_ref[2 * n + j] = acc_s[2 * n + j].astype(BF).T

        lax.fori_loop(0, n, out, None)
        dwo_ref[ALL] = acc_o[ALL].astype(BF)


def ffn_bwd(h, o, dy, wo, wg, wu, wd, number, projected, bt=512):
    t, d = h.shape
    f = wg.shape[2]
    blocks = 3 * f // FC
    every = blocks + 4
    return pl.pallas_call(
        functools.partial(_ffn_bwd_kernel, projected=projected),
        grid=(t // bt,),
        in_specs=[_rows(bt, d)] * 3 + [_of_layer(w, number) for w in (wo, wg, wu, wd)],
        out_specs=[_rows(bt, d), _rows(bt, d), pl.BlockSpec((8, bt), lambda i: (0, i)), _all((blocks, d, FC)), _all((d, d))],
        out_shape=[jax.ShapeDtypeStruct((t, d), BF), jax.ShapeDtypeStruct((t, d), BF), jax.ShapeDtypeStruct((8, t), F32),
                   jax.ShapeDtypeStruct((every, d, FC), BF), jax.ShapeDtypeStruct((d, d), BF)],
        scratch_shapes=[pltpu.VMEM((bt, d), F32), pltpu.VMEM((blocks, d, FC), F32), pltpu.VMEM((d, d), F32)],
        compiler_params=_params("arbitrary"),
        cost_estimate=_cost(16 * t * d * f + 6 * t * d * d, h, o, dy, h, h, wg, wg, wg, wg),
        name="ffn_bwd",
    )(h, o, dy, wo, wg, wu, wd)


def _qkv_bwd_kernel(h_ref, dh2_ref, cos_ref, sin_ref, dq_ref, dk_ref, dv_ref, dwo_ref, wq_ref, wk_ref, wv_ref, _, *rest, needs_dh):
    dh_ref, (grad_ref, acc_s) = (rest[0], rest[1:]) if needs_dh else (None, rest)
    i, steps = pl.program_id(0), pl.num_programs(0)

    @pl.when(i == 0)
    def _():
        acc_s[ALL] = jnp.zeros_like(acc_s)

    wide, scale, a = _norm(h_ref[ALL])
    cos, sin = cos_ref[ALL], -sin_ref[ALL]
    dq = _turn(dq_ref[ALL].astype(F32), cos, sin).astype(BF)
    dk = _turn(dk_ref[ALL].astype(F32), cos, sin).astype(BF)
    dv = dv_ref[ALL]
    a_t = a.T
    acc_s[0] += _mm(a_t, dq)
    acc_s[1] += _mm(a_t, dk)
    acc_s[2] += _mm(a_t, dv)
    if needs_dh:
        da = _by_rows(dq, wq_ref[ALL]) + _by_rows(dk, wk_ref[ALL]) + _by_rows(dv, wv_ref[ALL])
        back = _norm_bwd(wide, scale, da.astype(BF).astype(F32)).astype(BF)
        dh_ref[ALL] = (dh2_ref[ALL].astype(F32) + back.astype(F32)).astype(BF)

    @pl.when(i == steps - 1)
    def _():
        for k in range(3):
            grad_ref[k] = acc_s[k].astype(BF)
        grad_ref[3] = dwo_ref[ALL]


def qkv_bwd(h, dh2, cos, sin, dq, dk, dv, dwo, wq, wk, wv, grads, number, needs_dh, bt=512):
    t, d = h.shape
    last = grads.shape[0] // 4 - 1
    got = pl.pallas_call(
        functools.partial(_qkv_bwd_kernel, needs_dh=needs_dh),
        grid=(t // bt,),
        in_specs=[_rows(bt, d), _rows(bt, d), _rows(bt, HEAD), _rows(bt, HEAD)] + [_rows(bt, d)] * 3 + [_all((d, d))]
        + [_of_layer(w, number) for w in (wq, wk, wv)] + [pl.BlockSpec(memory_space=pl.ANY)],
        out_specs=[_rows(bt, d)] * needs_dh + [pl.BlockSpec((4, d, d), lambda i: (last, 0, 0))],
        out_shape=[jax.ShapeDtypeStruct((t, d), BF)] * needs_dh + [jax.ShapeDtypeStruct(grads.shape, BF)],
        input_output_aliases={11: int(needs_dh)},
        scratch_shapes=[pltpu.VMEM((3, d, d), F32)],
        compiler_params=_params("arbitrary"),
        cost_estimate=_cost((6 + 6 * needs_dh) * t * d * d, h, h, h, h, h, h, wq),
        name="qkv_bwd",
    )(h, dh2, cos, sin, dq, dk, dv, dwo, wq, wk, wv, grads)
    return got if needs_dh else (None, *got)


STEPS = 8


def _adamw_kernel(f_ref, *refs):
    factor = f_ref[0, 0]
    grads, ins, outs = refs[:4], refs[4:25], refs[-21:]
    for n in range(7):
        (w_ref, m_ref, v_ref), (nw_ref, nm_ref, nv_ref) = ins[n::7], outs[n::7]
        g = (grads[3][n] if n < 4 else grads[n - 4][ALL]).astype(F32) * factor
        m = 0.9 * m_ref[ALL] + 0.1 * g
        v = 0.95 * v_ref[ALL] + 0.05 * g * g
        w = w_ref[ALL].astype(F32)
        nw_ref[ALL] = (w - 0.02 * (m * lax.rsqrt(v + 1e-8) + 0.1 * w)).astype(BF)
        nm_ref[ALL] = m
        nv_ref[ALL] = v


def adamw(factor, grads, arrays, layer, into):
    d = arrays[0].shape[1]
    per = arrays[4].shape[2] // FC
    cut = STEPS // per
    rows, few = d // cut, d // STEPS
    wide = lambda n: pl.BlockSpec((None, rows, FC), lambda j: (n * per + j // cut, j % cut, 0))
    blocks = [wide(0), wide(1), wide(2), pl.BlockSpec((4, few, FC), lambda j: (3 * per // 4, j, 0))]
    small = pl.BlockSpec((None, few, d), lambda j: (layer, j, 0))
    across = pl.BlockSpec((None, rows, FC), lambda j: (layer, j % cut, j // cut))
    down = pl.BlockSpec((None, rows, FC), lambda j: (layer, j, 0))
    specs = ([small] * 4 + [across] * 2 + [down]) * 3
    first = 1 + len(blocks) + len(arrays)
    return pl.pallas_call(
        _adamw_kernel,
        grid=(STEPS,),
        in_specs=[pl.BlockSpec(memory_space=pltpu.SMEM)] + blocks + specs + [pl.BlockSpec(memory_space=pl.ANY)] * len(into),
        out_specs=specs,
        out_shape=[jax.ShapeDtypeStruct(a.shape, a.dtype) for a in arrays],
        input_output_aliases={first + n: n for n in range(len(into))},
        compiler_params=_params("arbitrary"),
        cost_estimate=_cost(10**10, *arrays),
        name="adamw",
    )(factor, *[grads] * 4, *arrays, *into)


ZS = 4
GROUP = 32
PARTS = 2


def _coords():
    i = lax.axis_index("dp")
    return i // 16, i // 8 % 2, i // 2 % 4, i % 2


def _number(x, y, z, c):
    return ((x * 2 + y) * ZS + z) * 2 + c


def _copy(src, dst, send, recv, to):
    return pltpu.make_async_remote_copy(src_ref=src, dst_ref=dst, send_sem=send, recv_sem=recv, device_id={"dp": to},
                                        device_id_type=pl.DeviceIdType.MESH)


def _add(out, *terms):
    step = 32

    def some(k, _):
        at = pl.ds(pl.multiple_of(k * step, step), step)
        total = terms[0][at, :].astype(F32)
        for t in terms[1:]:
            total += t[at, :].astype(F32)
        out[at, :] = total.astype(BF)

    lax.fori_loop(0, out.shape[0] // step, some, None)


class _Scatter:
    @staticmethod
    def scratch(rows, n):
        b = rows // 16
        sem = pltpu.SemaphoreType.DMA
        return [pltpu.VMEM((8, b, n), BF), pltpu.VMEM((8, b, n), BF), pltpu.VMEM((4, b, n), BF), pltpu.VMEM((2, b, n), BF),
                pltpu.VMEM((6, b // ZS, n), BF), sem((8,)), sem((8,)), sem((8,)), sem((4,)), sem((4,)), sem((2,)), sem((2,)), sem((6,)), sem((6,))]

    def __init__(self, g_ref, share_ref, refs):
        (self.own, self.rc, self.ra, self.rb, self.rz, local, cs, cr, as_, ar, bs, br, zs, zr) = refs
        self.share = share_ref
        x, y, z, c = _coords()
        self.z, self.r = z, g_ref.shape[0] // 64
        b = ZS * self.r
        peer = {"x": _number(1 - x, y, z, c), "y": _number(x, 1 - y, z, c), "c": _number(x, y, z, 1 - c)}
        place = lambda c, h, x, y: g_ref.at[pl.ds(pl.multiple_of((((c * 2 + h) * 2 + x) * 2 + y) * b, b), b)]
        self.local, self.core = [], []
        for n in range(8):
            h, first, second = n // 4, n // 2 % 2, n % 2
            dx, dy = (first, second) if h == 0 else (second, first)
            bx, by = (x + dx) % 2, (y + dy) % 2
            self.local.append(pltpu.make_async_copy(place(c, h, bx, by), self.own.at[n], local.at[n]))
            self.core.append(_copy(place(1 - c, h, bx, by), self.rc.at[n], cs.at[n], cr.at[n], peer["c"]))
        axes = ("xy", "yx")
        self.a = [_copy(self.own.at[h * 4 + 2 + s], self.ra.at[h * 2 + s], as_.at[h * 2 + s], ar.at[h * 2 + s], peer[axes[h][0]])
                  for h in range(2) for s in range(2)]
        self.b = [_copy(self.own.at[h * 4 + 1], self.rb.at[h], bs.at[h], br.at[h], peer[axes[h][1]]) for h in range(2)]
        self.zc = []
        for h in range(2):
            for k in (1, 2, 3):
                to = (z + k) % ZS
                n = h * 3 + k - 1
                self.zc.append(_copy(self.own.at[h * 4, pl.ds(pl.multiple_of(to * self.r, self.r), self.r)], self.rz.at[n], zs.at[n], zr.at[n],
                                     _number(x, y, to, c)))

    def start(self):
        for n in (2, 6, 3, 7, 1, 5, 0, 4):
            self.core[n].start()
            self.local[n].start()

    def _core(self, n):
        self.core[n].wait_recv()
        self.local[n].wait()
        _add(self.own.at[n], self.own.at[n], self.rc.at[n])

    def first(self):
        for s in (1, 0):
            for h in (0, 1):
                self._core(h * 4 + 2 + s)
                self.a[h * 2 + s].start()

    def keep(self):
        for n in (1, 5, 0, 4):
            self._core(n)

    def second(self):
        for h in (0, 1):
            self.a[h * 2 + 1].wait_recv()
            _add(self.own.at[h * 4 + 1], self.own.at[h * 4 + 1], self.ra.at[h * 2 + 1])
            self.b[h].start()

    def third(self):
        for h in (0, 1):
            self.a[h * 2].wait_recv()
            self.b[h].wait_recv()
            mine = self.own.at[h * 4]
            _add(mine, mine, self.ra.at[h * 2], self.rb.at[h])
            for k in (0, 1, 2):
                self.zc[h * 3 + k].start()

    def last(self):
        for h in (0, 1):
            for k in (0, 1, 2):
                self.zc[h * 3 + k].wait_recv()
            mine = self.own.at[h * 4, pl.ds(pl.multiple_of(self.z * self.r, self.r), self.r)]
            _add(self.share.at[pl.ds(h * self.r, self.r)], mine, *[self.rz.at[h * 3 + k] for k in (0, 1, 2)])
        for copy in self.core + self.a + self.b + self.zc:
            copy.wait_send()

    def phases(self):
        return [self.start, self.first, self.keep, self.second, self.third, self.last]


def _scatter_kernel(g_ref, s_ref, *refs):
    per = len(_Scatter.scratch(1024, HEAD))
    rows, own = g_ref.shape[0] // PARTS, s_ref.shape[0] // PARTS
    part = [_Scatter(g_ref.at[pl.ds(k * rows, rows)], s_ref.at[pl.ds(k * own, own)], refs[k * per : (k + 1) * per]) for k in range(PARTS)]
    for p in part:
        p.start()
    for t in range(PARTS + 2):
        if t < PARTS:
            part[t].first()
        if 0 <= t - 1 < PARTS:
            part[t - 1].keep()
            part[t - 1].second()
        if 0 <= t - 2 < PARTS:
            part[t - 2].third()
    for p in part:
        p.last()


def scattered_sum(g):
    rows, n = g.shape
    return pl.pallas_call(
        _scatter_kernel,
        in_specs=[pl.BlockSpec(memory_space=pl.ANY)],
        out_specs=pl.BlockSpec(memory_space=pltpu.VMEM),
        out_shape=jax.ShapeDtypeStruct((rows // GROUP, n), BF),
        scratch_shapes=_Scatter.scratch(rows // PARTS, n) * PARTS,
        compiler_params=pltpu.CompilerParams(vmem_limit_bytes=VMEM, has_side_effects=True),
        cost_estimate=pl.CostEstimate(flops=10**10, transcendentals=0, bytes_accessed=10**7),
        name="scatter",
    )(g)


class _Gather:
    @staticmethod
    def scratch():
        sem = pltpu.SemaphoreType.DMA
        return [sem((2,)), sem((6,)), sem((6,)), sem((8,)), sem((8,)), sem((16,)), sem((16,)), sem((32,)), sem((32,))]

    def __init__(self, share_ref, out_ref, refs):
        local, zs, zr, ss, sr, ts, tr, cs, cr = refs
        x, y, z, c = _coords()
        r = share_ref.shape[0] // 2
        where = lambda h, x, y, z: out_ref.at[pl.ds(pl.multiple_of(((((c * 2 + h) * 2 + x) * 2 + y) * ZS + z) * r, r), r)]
        to_x, to_y, to_c = _number(1 - x, y, z, c), _number(x, 1 - y, z, c), _number(x, y, z, 1 - c)
        self.local, self.z, self.s, self.t, self.c = [], {}, {}, {}, {}
        for h in range(2):
            own = share_ref.at[pl.ds(h * r, r)]
            self.local.append(pltpu.make_async_copy(own, where(h, x, y, z), local.at[h]))
            for k in (1, 2, 3):
                n = h * 3 + k - 1
                self.z[h, k] = _copy(own, where(h, x, y, z), zs.at[n], zr.at[n], _number(x, y, (z + k) % ZS, c))
            for k in range(4):
                bz = (z + ZS - k) % ZS
                near = where(h, x, y, bz)
                src = own if k == 0 else near
                n = h * 4 + k
                self.s[h, k] = _copy(src, near, ss.at[n], sr.at[n], (to_y, to_x)[h])
                for side in range(2):
                    far = near if side == 0 else (where(0, x, 1 - y, bz), where(1, 1 - x, y, bz))[h]
                    n = (h * 4 + k) * 2 + side
                    self.t[h, k, side] = _copy(src if side == 0 else far, far, ts.at[n], tr.at[n], (to_x, to_y)[h])
                for side in range(4):
                    at = where(h, (x, x, 1 - x, 1 - x)[side] if h == 0 else (x, 1 - x, x, 1 - x)[side],
                               (y, 1 - y, y, 1 - y)[side] if h == 0 else (y, y, 1 - y, 1 - y)[side], bz)
                    n = (h * 4 + k) * 4 + side
                    self.c[h, k, side] = _copy(src if side == 0 else at, at, cs.at[n], cr.at[n], to_c)

    def _near(self, h, k):
        self.s[h, k].start()
        self.t[h, k, 0].start()
        self.c[h, k, 0].start()

    def start(self):
        for h in (0, 1):
            self.local[h].start()
            for k in (2, 1, 3):
                self.z[h, k].start()
            self._near(h, 0)

    def first(self):
        for k in (2, 1, 3):
            for h in (0, 1):
                self.z[h, k].wait_recv()
                self._near(h, k)

    def second(self):
        for k in (0, 2, 1, 3):
            for h in (0, 1):
                self.s[h, k].wait_recv()
                self.t[h, k, 1].start()
                self.c[h, k, 1].start()

    def third(self):
        for side in (0, 1):
            for k in (0, 2, 1, 3):
                for h in (0, 1):
                    self.t[h, k, side].wait_recv()
                    self.c[h, k, 2 + side].start()

    def last(self):
        for copy in self.c.values():
            copy.wait_recv()
        for copies in (self.z, self.s, self.t, self.c):
            for copy in copies.values():
                copy.wait_send()
        for copy in self.local:
            copy.wait()

    def phases(self):
        return [self.start, self.first, self.second, self.third, self.last]


def _gather_kernel(s_ref, other_ref, g_ref, sum_ref, all_ref, send, recv, *refs):
    per = len(_Gather.scratch())
    rows, own = g_ref.shape[0] // PARTS, s_ref.shape[0] // PARTS
    part = [_Gather(s_ref.at[pl.ds(k * own, own)], g_ref.at[pl.ds(k * rows, rows)], refs[k * per : (k + 1) * per]) for k in range(PARTS)]
    for p in part:
        p.start()

    def squares(ref, total):
        def some(k, total):
            g = ref[pl.ds(pl.multiple_of(k * 8, 8), 8), :].astype(F32)
            g = g * g
            for at in range(0, ref.shape[1], HEAD):
                total = total + g[:, at : at + HEAD]
            return total

        return lax.fori_loop(0, ref.shape[0] // 8, some, total)

    me = lax.axis_index("dp")
    none = jnp.zeros(sum_ref.shape, F32)
    all_ref[me] = squares(other_ref, squares(s_ref, none))

    def told(k):
        return _copy(all_ref.at[me], all_ref.at[me], send.at[k], recv.at[k], (me + k) % GROUP)

    lax.fori_loop(1, GROUP, lambda k, _: told(k).start(), None)
    for p in part:
        p.first()
    for p in part:
        p.second()
    lax.fori_loop(1, GROUP, lambda k, _: told(k).wait_recv(), None)
    sum_ref[ALL] = lax.fori_loop(0, GROUP, lambda k, t: t + all_ref[k], none)
    for p in part:
        p.third()
    for p in part:
        p.last()
    lax.fori_loop(1, GROUP, lambda k, _: told(k).wait_send(), None)


def gathered(s, other):
    rows, n = s.shape
    vmem = pl.BlockSpec(memory_space=pltpu.VMEM)
    sem = pltpu.SemaphoreType.DMA((GROUP,))
    return pl.pallas_call(
        _gather_kernel,
        in_specs=[vmem, vmem],
        out_specs=[pl.BlockSpec(memory_space=pl.ANY), vmem],
        out_shape=[jax.ShapeDtypeStruct((rows * GROUP, n), BF), jax.ShapeDtypeStruct((8, HEAD), F32)],
        scratch_shapes=[pltpu.VMEM((GROUP, 8, HEAD), F32), sem, sem] + _Gather.scratch() * PARTS,
        compiler_params=pltpu.CompilerParams(vmem_limit_bytes=VMEM, has_side_effects=True),
        cost_estimate=pl.CostEstimate(flops=10**10, transcendentals=0, bytes_accessed=10**7),
        name="gather",
    )(s, other)


def solution(mesh):
    def step(x, dy, *arrays):
        weights = arrays[:7]
        wq, wk, wv, wo, wg, wu, wd = weights
        layers = wq.shape[0]
        h, dh = x[0], dy[0]
        lane, tokens = jnp.arange(HEAD), h.shape[0]
        rate = THETA ** (-(lane % (HEAD // 2)).astype(F32) / (HEAD // 2))
        far, near = jnp.arange(0, tokens, 64, dtype=F32)[:, None] * rate, jnp.arange(64, dtype=F32)[:, None] * rate
        sign = jnp.where(lane < HEAD // 2, -1.0, 1.0)
        cf, sf, cn, sn = lax.optimization_barrier((jnp.cos(far), jnp.sin(far), jnp.cos(near), jnp.sin(near)))
        cf, sf = cf[:, None], sf[:, None]
        cos = (cf * cn - sf * sn).reshape(tokens, HEAD)
        sin = ((sf * cn + cf * sn) * sign).reshape(tokens, HEAD)
        kept = []
        for n in range(layers):
            q, k, val = qkv(h, cos, sin, wq, wk, wv, n)
            o, lse = attend(q, k, val)
            if n < layers - 1:
                h2, h3 = ffn(h, o, wo, wg, wu, wd, n)
            else:
                h2, h3 = h, None
            kept.append((h, q, k, val, o, lse, h2))
            h = h3
        grads = [None] * layers
        for n in reversed(range(layers)):
            h, q, k, val, o, lse, h2 = kept[n]
            dh2, do, delta, some, dwo = ffn_bwd(h2, o, dh, wo, wg, wu, wd, n, n < layers - 1)
            dq, dk, dval = attend_bwd(q, k, val, do, lse, delta)
            dh, grads[n] = qkv_bwd(h, dh2, cos, sin, dq, dk, dval, dwo, wq, wk, wv, some, n, n > 0)
            if n == 1:
                s1 = lax.psum_scatter(grads[1].reshape(-1, FC), "dp", scatter_dimension=0, tiled=True)
        shape = grads[0].shape
        s0 = scattered_sum(grads[0].reshape(-1, FC))
        g1 = lax.all_gather(s1, "dp", axis=0, tiled=True)
        g0, squares = gathered(s0, s1)
        count = sum(w.size for w in weights)
        factor = jnp.minimum(1.0, 0.5 * lax.rsqrt(jnp.sum(squares) / count + 1e-30)).reshape(1, 1)
        new = ()
        for n, g in enumerate((g0, g1)):
            new = adamw(factor, g.reshape(shape), arrays, n, new)
        return tuple(new)

    states, all_of = P(("rep", "dp"), None, None), P(None, None, None)
    return jax.shard_map(
        step,
        mesh=mesh,
        in_specs=(states, states) + (all_of,) * 21,
        out_specs=(P("rep", None, None),) * 21,
        check_vma=False,
    )
```
